32 devices in a mesh: dp: 8 (over z, x), mp: 4 (over y, core).
Axes of the slice: x: 2, y: 2, z: 4, core: 2. Of those that a mesh axis runs over, the one named last changes fastest.
Arguments:
- query_emb: bfloat16 [2048, 768], P('dp'), may hold values from -6 to 6
- positive_list: int32 [2048], replicated, may hold values from 0 to 32767
- centroids: float32 [32768, 768], P(('dp', 'mp')), may hold values from -0.6 to 0.6
- first_moment: float32 [32768, 768], P(('dp', 'mp')), may hold values from -3 to 3
- second_moment: float32 [32768, 768], P(('dp', 'mp')), may hold values from 0.05 to 2
Outputs:
- new_centroids: float32 [32768, 768], P(('dp', 'mp'))
- new_first: float32 [32768, 768], P(('dp', 'mp'))
- new_second: float32 [32768, 768], P(('dp', 'mp'))
- mean_loss: float32 [], replicated
The draws below stay inside these ranges and needn't reach their ends.
All inputs are finite; a program needn't handle non-finite values.
Results may differ from the reference program's by a relative error of at most 0.00097.
Values may be sent and summed in bfloat16 or wider, within the bound.
A program may use at most 64 MiB of HBM per device.

```python
import math
import jax
import jax.numpy as jnp
from jax import lax

D = 768
LISTS = 32768
ROWS = 2048


def centroid_rows(key):
    base_scale = 3.5 / math.sqrt(D)
    base = jnp.clip(base_scale * jax.random.normal(key, (LISTS, D), jnp.float32), -0.6, 0.6)
    signs = jnp.where(jax.random.normal(jax.random.fold_in(key, 3), (LISTS, D), jnp.float32) >= 0.0, base_scale, -base_scale)
    list_ids = jnp.arange(LISTS, dtype=jnp.int32)
    peaked = (list_ids % 1024 == 5)[:, None]
    return jnp.where(peaked, signs, base)


def draw_centroids(key, part):
    return centroid_rows(jax.random.fold_in(key, 11))


def draw_query_emb(key, part):
    base_scale = 3.5 / math.sqrt(D)
    aligned_size = min(6.0, 290.0 / (base_scale * D))
    table_full = centroid_rows(jax.random.fold_in(key, 11))
    noise_key = jax.random.fold_in(key, 12)
    background = jnp.clip(jax.random.normal(noise_key, (ROWS, D), jnp.float32), -6.0, 6.0)
    row_ids = jnp.arange(ROWS, dtype=jnp.int32)
    picked = (row_ids // 64 * 1024 + 5) % LISTS
    aligned = aligned_size * jnp.sign(table_full[picked])
    chosen = (row_ids % 64 == 0)[:, None]
    values = jnp.where(chosen, aligned, background)
    return values.astype(jnp.bfloat16)


def set_ends(array, stream_key, least, top_value):
    place = [jax.random.randint(jax.random.fold_in(stream_key, axis), (), 0, length) for axis, length in enumerate(array.shape)]
    widest = array.shape.index(max(array.shape))
    neighbour = place[:widest] + [(place[widest] + 1) % array.shape[widest]] + place[widest + 1:]
    return array.at[tuple(place)].set(least).at[tuple(neighbour)].set(top_value)


def block_levels(rng, extent, shards, smallest, high):
    level, own = 1.0, jax.random.fold_in(rng, 6)
    for axis_at, blocks in shards:
        heights = jnp.exp(jax.random.uniform(jax.random.fold_in(own, axis_at), (blocks,), jnp.float32, smallest / len(shards), high / len(shards)))
        level = level * jnp.repeat(heights, extent[axis_at] // blocks).reshape([-1 if axis == axis_at else 1 for axis in range(len(extent))])
    return level


def normal_values(own_key, extent, width, bound, cuts=(), kind=jnp.bfloat16):
    drawn = width * jax.random.normal(own_key, extent, jnp.float32)
    if cuts:
        drawn = drawn * block_levels(own_key, extent, cuts, -0.22, 0.18)
    return jnp.clip(drawn, -bound, bound).astype(kind)


def setup_inputs(seed: int = 0) -> dict:
    key_of = jax.random.split(jax.random.key(seed), 6)
    query_emb = draw_query_emb(jax.random.fold_in(key_of[5], 71), 0)
    positive_list = set_ends(jax.random.randint(key_of[1], (ROWS,), 0, LISTS), jax.random.fold_in(key_of[1], 1), 0, LISTS - 1).astype(jnp.int32)
    centroids = draw_centroids(jax.random.fold_in(key_of[5], 71), 0)
    first_moment = normal_values(key_of[3], (LISTS, D), 0.5, 3.0, ((0, 32),), jnp.float32)
    second_moment = jnp.clip(jnp.exp(math.log(2.0) - 3.6888794 * jax.random.uniform(key_of[4], (LISTS, D), jnp.float32) ** block_levels(key_of[4], (LISTS, D), ((0, 32),), -0.2, 0.2)), 0.05, 2.0)
    return {"query_emb": query_emb, "positive_list": positive_list, "centroids": centroids, "first_moment": first_moment, "second_moment": second_moment}


beta_first = 0.9
beta_second = 0.95
learn_rate = 0.01
epsilon = 1e-08

def adam_update(centroids, first_moment, second_moment, gradient):
    new_first = beta_first * first_moment + (1.0 - beta_first) * gradient
    new_second = beta_second * second_moment + (1.0 - beta_second) * gradient * gradient
    new_centroids = centroids - learn_rate * new_first / (jnp.sqrt(new_second) + epsilon)
    return (new_centroids, new_first, new_second)

def reference(query_emb, positive_list, centroids, first_moment, second_moment):
    table_half = centroids.astype(jnp.bfloat16)
    block_rows = math.gcd(ROWS, 512)
    query_blocks = query_emb.reshape(ROWS // block_rows, block_rows, D)
    target_blocks = positive_list.reshape(ROWS // block_rows, block_rows)
    list_ids = jnp.arange(LISTS, dtype=jnp.int32)

    def scan_step(state_pair, block_item):
        gradient, loss_sum = state_pair
        queries, targets = block_item
        logits = jnp.dot(queries, table_half.T, preferred_element_type=jnp.float32)
        row_peak = lax.optimization_barrier(jnp.max(logits, axis=1))
        row_mass = lax.optimization_barrier(jnp.sum(jnp.exp(logits - row_peak[:, None]), axis=1))
        log_norm = row_peak + jnp.log(row_mass)
        is_target = list_ids[None, :] == targets[:, None].astype(jnp.int32)
        row_target = lax.optimization_barrier(jnp.sum(jnp.where(is_target, logits, jnp.zeros_like(logits)), axis=1))
        loss_sum = loss_sum + jnp.sum(log_norm - row_target)
        weights = (jnp.exp(logits - log_norm[:, None]) - is_target.astype(jnp.float32)).astype(jnp.bfloat16)
        gradient = gradient + jnp.dot(weights.T, queries, preferred_element_type=jnp.float32)
        return ((gradient, loss_sum), None)
    start_state = (jnp.zeros((LISTS, D), jnp.float32), jnp.zeros((), jnp.float32))
    final_state, unused = lax.scan(scan_step, start_state, (query_blocks, target_blocks))
    gradient, loss_sum = final_state
    new_centroids, new_first, new_second = adam_update(centroids, first_moment, second_moment, gradient)
    return (new_centroids, new_first, new_second, loss_sum / ROWS)
```

```python
import functools

import jax
import jax.numpy as jnp
from jax import lax
from jax.experimental import pallas as pl
from jax.experimental.pallas import tpu as pltpu
from jax.sharding import PartitionSpec as P

beta_first = 0.9
beta_second = 0.95
learn_rate = 0.01
epsilon = 1e-08

MESH = pl.DeviceIdType.MESH


def adam_update(centroids, first_moment, second_moment, gradient):
    new_first = beta_first * first_moment + (1.0 - beta_first) * gradient
    new_second = beta_second * second_moment + (1.0 - beta_second) * gradient * gradient
    new_centroids = centroids - learn_rate * new_first / (jnp.sqrt(new_second) + epsilon)
    return (new_centroids, new_first, new_second)


def merge_stages(count_dp, count_mp):
    bits = [("mp", 1 << b) for b in range(count_mp.bit_length() - 1)]
    bits += [("dp", 1 << b) for b in range(count_dp.bit_length() - 1)]
    stages = [bits[:1]]
    for at in range(1, len(bits), 2):
        stages.append(bits[at : at + 2])
    return [
        [stage[:1]] if len(stage) == 1 else [stage[:1], stage[1:], stage] for stage in stages
    ]


def flip(index, bit):
    return index + (1 - 2 * lax.rem(lax.div(index, bit), 2)) * bit


def log_add(values):
    top = functools.reduce(jnp.maximum, values)
    terms = [jnp.exp(value - top) for value in values]
    while len(terms) > 1:
        terms = [terms[i] + terms[i + 1] for i in range(0, len(terms), 2)]
    return top + jnp.log(terms[0])


def plain_add(terms):
    while len(terms) > 1:
        terms = [terms[i] + terms[i + 1] for i in range(0, len(terms), 2)]
    return terms[0]


def kernel(
    n,
    count_mp,
    stages,
    q_ref,
    pos_ref,
    cent_ref,
    grad_ref,
    loss_ref,
    rows_all,
    logits,
    cent,
    table,
    weights,
    stats,
    landed,
    cent_sem,
    ring_send,
    ring_recv,
    pair_send,
    pair_recv,
    stat_send,
    stat_recv,
):
    R, D = q_ref.shape
    K = cent_ref.shape[0]
    half = R // 2
    piece = half // 2
    dp = lax.axis_index("dp")
    mp = lax.axis_index("mp")
    core = lax.rem(mp, 2)
    other = mp + 1 - 2 * core
    odd = lax.rem(dp, 2)
    place = (1 - odd) * lax.div(dp, 2) + odd * (n - 1 - lax.div(dp, 2))

    def at_place(p):
        back = lax.div(p, n // 2)
        return (1 - back) * 2 * p + back * (2 * (n - 1 - p) + 1)

    right = at_place(lax.rem(place + 1, n))
    left = at_place(lax.rem(place + n - 1, n))

    cent_copy = pltpu.make_async_copy(cent_ref, cent, cent_sem)
    cent_copy.start()

    def peer(mask):
        ids = {"dp": dp, "mp": mp}
        for axis, bit in mask:
            ids[axis] = flip(ids[axis], bit)
        return ids

    greeted = [{"dp": left, "mp": mp}, {"dp": right, "mp": mp}]
    greeted += [peer(mask) for stage in stages for mask in stage]
    barrier = pltpu.get_barrier_semaphore()
    for device in greeted:
        pl.semaphore_signal(barrier, inc=1, device_id=device, device_id_type=MESH)
    pl.semaphore_wait(barrier, len(greeted))

    def rows(origin, which, p):
        start = pl.multiple_of(origin * R + which * half + p * piece, piece)
        return rows_all.at[pl.ds(start, piece)]

    def ring_copy(src, origin, j, p, target):
        return pltpu.make_async_remote_copy(
            src_ref=src,
            dst_ref=rows(origin, core, p),
            send_sem=ring_send.at[j, p],
            recv_sem=ring_recv.at[j, p],
            device_id={"dp": target, "mp": mp},
            device_id_type=MESH,
        )

    def pair_copy(origin, j, p, which):
        block = rows(origin, which, p)
        return pltpu.make_async_remote_copy(
            src_ref=block,
            dst_ref=block,
            send_sem=pair_send.at[j, p],
            recv_sem=pair_recv.at[j, p],
            device_id={"dp": dp, "mp": other},
            device_id_type=MESH,
        )

    for p in range(2):
        own = q_ref.at[pl.ds(pl.multiple_of(core * half + p * piece, piece), piece)]
        ring_copy(own, dp, 1, p, right).start()
        ring_copy(own, dp, 2, p, left).start()

    base = (dp * count_mp + mp) * K
    first = stats.at[0]
    first[pl.ds(n, 8), :] = jnp.zeros((8, R), jnp.float32)

    def is_target(origin, start, size):
        local = pos_ref[pl.ds(origin, 1), :] - (base + start)
        return lax.broadcasted_iota(jnp.int32, (size, R), 0) == local

    step_rows = min(K, 256)

    def forward(origin):
        block = rows_all[pl.ds(pl.multiple_of(origin * R, R), R), :]
        found = lax.dot_general(
            table[...], block, (((1,), (1,)), ((), ())), preferred_element_type=jnp.float32
        )
        logits[origin] = found
        peak = jnp.max(found, axis=0, keepdims=True)
        mass = jnp.zeros((1, R), jnp.float32)
        target = jnp.zeros((1, R), jnp.float32)
        for start in range(0, K, step_rows):
            part = logits[origin, pl.ds(start, step_rows), :]
            mass += jnp.sum(jnp.exp(part - peak), axis=0, keepdims=True)
            target += jnp.sum(
                jnp.where(is_target(origin, start, step_rows), part, 0.0), axis=0, keepdims=True
            )
        first[pl.ds(origin, 1), :] = peak + jnp.log(mass)
        first[pl.ds(n, 1), :] += target

    rows_all[pl.ds(pl.multiple_of(dp * R, R), R), :] = q_ref[...]
    cent_copy.wait()
    for start in range(0, K, step_rows):
        table[pl.ds(start, step_rows), :] = cent[pl.ds(start, step_rows), :].astype(jnp.bfloat16)

    forward(dp)
    far = n // 2

    def ring_step(d, carry):
        from_left = at_place(lax.rem(place - d + n, n))
        from_right = at_place(lax.rem(place + d, n))
        jl, jr = 2 * d - 1, 2 * d
        for p in range(2):
            block = rows(from_left, core, p)
            ring_copy(block, from_left, jl, p, right).wait_recv()
            onward = ring_copy(block, from_left, 2 * d + 1, p, right)
            if p == 0:
                onward.start()
            else:
                pl.when(d + 1 < far)(onward.start)
            pair_copy(from_left, jl, p, core).start()

            block = rows(from_right, core, p)
            ring_copy(block, from_right, jr, p, left).wait_recv()
            onward = ring_copy(
                block, from_right, 2 * d + 2 - p * lax.div(d + 1, far), p, left
            )
            if p == 1:
                onward.start()
            else:
                pl.when(d + 1 < far)(onward.start)
            pair_copy(from_right, jr, p, core).start()
        for p in range(2):
            pair_copy(from_left, jl, p, 1 - core).wait_recv()
            pair_copy(from_right, jr, p, 1 - core).wait_recv()
        forward(from_left)
        forward(from_right)
        return carry

    lax.fori_loop(1, far, ring_step, 0)

    last = at_place(lax.rem(place + far, n))
    for p in range(2):
        ring_copy(rows(last, core, p), last, n - 1, p, right).wait_recv()
        pair_copy(last, n - 1, p, core).start()
    for p in range(2):
        pair_copy(last, n - 1, p, 1 - core).wait_recv()
    forward(last)

    slot = 0
    for at, stage in enumerate(stages):
        copies = []
        for mask in stage:
            copies.append(
                pltpu.make_async_remote_copy(
                    src_ref=stats.at[at],
                    dst_ref=landed.at[slot],
                    send_sem=stat_send.at[slot],
                    recv_sem=stat_recv.at[slot],
                    device_id=peer(mask),
                    device_id_type=MESH,
                )
            )
            copies[-1].start()
            slot += 1
        for copy in copies:
            copy.wait_recv()
        held = [stats.at[at]] + [landed.at[slot - len(stage) + i] for i in range(len(stage))]
        merged = stats.at[at + 1]
        merged[pl.ds(0, n), :] = log_add([ref[pl.ds(0, n), :] for ref in held])
        merged[pl.ds(n, 8), :] = plain_add([ref[pl.ds(n, 8), :] for ref in held])
        for copy in copies:
            copy.wait_send()

    final = stats.at[len(stages)]
    loss = (jnp.sum(final[pl.ds(0, n), :]) - jnp.sum(final[pl.ds(n, 8), :])) * (1.0 / (n * R))
    loss_ref[...] = jnp.full(loss_ref.shape, loss, jnp.float32)

    chunk = weights.shape[0]

    def backward(i, carry):
        start = pl.multiple_of(i * chunk, chunk)
        for b in range(n):
            part = jnp.exp(logits[b, pl.ds(start, chunk), :] - final[pl.ds(b, 1), :])
            hit = is_target(b, start, chunk)
            weights[:, pl.ds(b * R, R)] = jnp.where(hit, part - 1.0, part).astype(jnp.bfloat16)
        grad_ref[pl.ds(start, chunk), :] = jnp.dot(
            weights[...], rows_all[...], preferred_element_type=jnp.float32
        )
        return carry

    lax.fori_loop(0, K // chunk, backward, 0)

    def drain(j, carry):
        for p in range(2):
            ring_copy(rows(dp, core, p), dp, j, p, right).wait_send()
            pair_copy(dp, j, p, core).wait_send()
        return carry

    lax.fori_loop(1, n, drain, 0)


def shards(query_emb, positive_list, centroids, first_moment, second_moment):
    n, count_mp = lax.axis_size("dp"), lax.axis_size("mp")
    R, D = query_emb.shape
    K = centroids.shape[0]
    stages = merge_stages(n, count_mp)
    slots = sum(len(stage) for stage in stages)
    chunk = min(K, 256)
    vmem = pl.BlockSpec(memory_space=pltpu.VMEM)
    gradient, loss = pl.pallas_call(
        functools.partial(kernel, n, count_mp, stages),
        out_shape=(
            jax.ShapeDtypeStruct((K, D), jnp.float32),
            jax.ShapeDtypeStruct((8, 128), jnp.float32),
        ),
        in_specs=[vmem, vmem, pl.BlockSpec(memory_space=pl.ANY)],
        out_specs=(vmem, vmem),
        scratch_shapes=[
            pltpu.VMEM((n * R, D), jnp.bfloat16),
            pltpu.VMEM((n, K, R), jnp.float32),
            pltpu.VMEM((K, D), jnp.float32),
            pltpu.VMEM((K, D), jnp.bfloat16),
            pltpu.VMEM((chunk, n * R), jnp.bfloat16),
            pltpu.VMEM((len(stages) + 1, n + 8, R), jnp.float32),
            pltpu.VMEM((slots, n + 8, R), jnp.float32),
            pltpu.SemaphoreType.DMA,
            pltpu.SemaphoreType.DMA((n, 2)),
            pltpu.SemaphoreType.DMA((n, 2)),
            pltpu.SemaphoreType.DMA((n, 2)),
            pltpu.SemaphoreType.DMA((n, 2)),
            pltpu.SemaphoreType.DMA((slots,)),
            pltpu.SemaphoreType.DMA((slots,)),
        ],
        compiler_params=pltpu.CompilerParams(
            collective_id=0, has_side_effects=True, vmem_limit_bytes=36 * 2**20
        ),
        cost_estimate=pl.CostEstimate(
            flops=4 * n * R * K * D, bytes_accessed=8 * K * D, transcendentals=2 * n * R * K
        ),
        name="gather_softmax_gradient",
    )(query_emb, positive_list.reshape(n, R), centroids)
    new_centroids, new_first, new_second = adam_update(
        centroids, first_moment, second_moment, gradient
    )
    return (new_centroids, new_first, new_second, loss[0, 0])


def solution(mesh):
    in_specs = (
        P("dp", None),
        P(),
        P(("dp", "mp"), None),
        P(("dp", "mp"), None),
        P(("dp", "mp"), None),
    )
    out_specs = (P(("dp", "mp"), None), P(("dp", "mp"), None), P(("dp", "mp"), None), P())
    return jax.shard_map(shards, mesh=mesh, in_specs=in_specs, out_specs=out_specs, check_vma=False)
```

```python
import functools

import jax
import jax.numpy as jnp
from jax import lax
from jax.experimental import pallas as pl
from jax.experimental.pallas import tpu as pltpu
from jax.sharding import PartitionSpec as P

beta_first = 0.9
beta_second = 0.95
learn_rate = 0.01
epsilon = 1e-08

MESH = pl.DeviceIdType.MESH


def adam_update(centroids, first_moment, second_moment, gradient):
    new_first = beta_first * first_moment + (1.0 - beta_first) * gradient
    new_second = beta_second * second_moment + (1.0 - beta_second) * gradient * gradient
    new_centroids = centroids - learn_rate * new_first / (jnp.sqrt(new_second) + epsilon)
    return (new_centroids, new_first, new_second)


def merge_stages(count_dp, count_mp):
    bits = [("mp", 1 << b) for b in range(count_mp.bit_length() - 1)]
    bits += [("dp", 1 << b) for b in range(count_dp.bit_length() - 1)]
    stages = [bits[:1]]
    for at in range(1, len(bits), 2):
        stages.append(bits[at : at + 2])
    return [
        [stage[:1]] if len(stage) == 1 else [stage[:1], stage[1:], stage] for stage in stages
    ]


def flip(index, bit):
    return index + (1 - 2 * lax.rem(lax.div(index, bit), 2)) * bit


def log_add(values):
    top = functools.reduce(jnp.maximum, values)
    terms = [jnp.exp(value - top) for value in values]
    while len(terms) > 1:
        terms = [terms[i] + terms[i + 1] for i in range(0, len(terms), 2)]
    return top + jnp.log(terms[0])


def plain_add(terms):
    while len(terms) > 1:
        terms = [terms[i] + terms[i + 1] for i in range(0, len(terms), 2)]
    return terms[0]


def kernel(
    n,
    count_mp,
    stages,
    q_ref,
    pos_ref,
    cent_ref,
    grad_ref,
    loss_ref,
    rows_all,
    logits,
    cent,
    table,
    weights,
    stats,
    landed,
    cent_sem,
    own_sem,
    ring_send,
    ring_recv,
    pair_send,
    pair_recv,
    stat_send,
    stat_recv,
):
    R, D = q_ref.shape
    K = cent_ref.shape[0]
    half = R // 2
    piece = half // 2
    dp = lax.axis_index("dp")
    mp = lax.axis_index("mp")
    core = lax.rem(mp, 2)
    other = mp + 1 - 2 * core
    odd = lax.rem(dp, 2)
    place = (1 - odd) * lax.div(dp, 2) + odd * (n - 1 - lax.div(dp, 2))

    def at_place(p):
        back = lax.div(p, n // 2)
        return (1 - back) * 2 * p + back * (2 * (n - 1 - p) + 1)

    right = at_place(lax.rem(place + 1, n))
    left = at_place(lax.rem(place + n - 1, n))

    cent_copy = pltpu.make_async_copy(cent_ref, cent, cent_sem)
    own_rows = rows_all.at[pl.ds(pl.multiple_of(dp * R, R), R)]
    own_copy = pltpu.make_async_copy(q_ref, own_rows, own_sem)
    own_copy.start()
    cent_copy.start()

    def peer(mask):
        ids = {"dp": dp, "mp": mp}
        for axis, bit in mask:
            ids[axis] = flip(ids[axis], bit)
        return ids

    greeted = [{"dp": left, "mp": mp}, {"dp": right, "mp": mp}]
    greeted += [peer(mask) for stage in stages for mask in stage]
    barrier = pltpu.get_barrier_semaphore()
    for device in greeted:
        pl.semaphore_signal(barrier, inc=1, device_id=device, device_id_type=MESH)
    pl.semaphore_wait(barrier, len(greeted))

    def rows(origin, which, p):
        start = pl.multiple_of(origin * R + which * half + p * piece, piece)
        return rows_all.at[pl.ds(start, piece)]

    def ring_copy(src, origin, j, p, target):
        return pltpu.make_async_remote_copy(
            src_ref=src,
            dst_ref=rows(origin, core, p),
            send_sem=ring_send.at[j, p],
            recv_sem=ring_recv.at[j, p],
            device_id={"dp": target, "mp": mp},
            device_id_type=MESH,
        )

    def pair_copy(origin, j, p, which):
        block = rows(origin, which, p)
        return pltpu.make_async_remote_copy(
            src_ref=block,
            dst_ref=block,
            send_sem=pair_send.at[j, p],
            recv_sem=pair_recv.at[j, p],
            device_id={"dp": dp, "mp": other},
            device_id_type=MESH,
        )

    own_copy.wait()
    for p in range(2):
        own = rows(dp, core, p)
        ring_copy(own, dp, 1, p, right).start()
        ring_copy(own, dp, 2, p, left).start()

    base = (dp * count_mp + mp) * K
    first = stats.at[0]
    first[pl.ds(n, 8), :] = jnp.zeros((8, R), jnp.float32)

    def is_target(origin, start, size):
        local = pos_ref[pl.ds(origin, 1), :] - (base + start)
        return lax.broadcasted_iota(jnp.int32, (size, R), 0) == local

    step_rows = min(K, 256)

    def forward(origin):
        block = rows_all[pl.ds(pl.multiple_of(origin * R, R), R), :]
        found = lax.dot_general(
            table[...], block, (((1,), (1,)), ((), ())), preferred_element_type=jnp.float32
        )
        logits[origin] = found
        peak = jnp.max(found, axis=0, keepdims=True)
        mass = jnp.zeros((1, R), jnp.float32)
        target = jnp.zeros((1, R), jnp.float32)
        for start in range(0, K, step_rows):
            part = logits[origin, pl.ds(start, step_rows), :]
            mass += jnp.sum(jnp.exp(part - peak), axis=0, keepdims=True)
            target += jnp.sum(
                jnp.where(is_target(origin, start, step_rows), part, 0.0), axis=0, keepdims=True
            )
        first[pl.ds(origin, 1), :] = peak + jnp.log(mass)
        first[pl.ds(n, 1), :] += target

    cent_copy.wait()
    for start in range(0, K, step_rows):
        table[pl.ds(start, step_rows), :] = cent[pl.ds(start, step_rows), :].astype(jnp.bfloat16)

    forward(dp)
    far = n // 2

    def ring_step(d, carry):
        from_left = at_place(lax.rem(place - d + n, n))
        from_right = at_place(lax.rem(place + d, n))
        jl, jr = 2 * d - 1, 2 * d
        for p in range(2):
            block = rows(from_left, core, p)
            ring_copy(block, from_left, jl, p, right).wait_recv()
            onward = ring_copy(block, from_left, 2 * d + 1, p, right)
            if p == 0:
                onward.start()
            else:
                pl.when(d + 1 < far)(onward.start)
            pair_copy(from_left, jl, p, core).start()

            block = rows(from_right, core, p)
            ring_copy(block, from_right, jr, p, left).wait_recv()
            onward = ring_copy(
                block, from_right, 2 * d + 2 - p * lax.div(d + 1, far), p, left
            )
            if p == 1:
                onward.start()
            else:
                pl.when(d + 1 < far)(onward.start)
            pair_copy(from_right, jr, p, core).start()
        for p in range(2):
            pair_copy(from_left, jl, p, 1 - core).wait_recv()
            pair_copy(from_right, jr, p, 1 - core).wait_recv()
        forward(from_left)
        forward(from_right)
        return carry

    lax.fori_loop(1, far, ring_step, 0)

    last = at_place(lax.rem(place + far, n))
    for p in range(2):
        ring_copy(rows(last, core, p), last, n - 1, p, right).wait_recv()
        pair_copy(last, n - 1, p, core).start()
    for p in range(2):
        pair_copy(last, n - 1, p, 1 - core).wait_recv()
    forward(last)

    slot = 0
    for at, stage in enumerate(stages):
        copies = []
        for mask in stage:
            copies.append(
                pltpu.make_async_remote_copy(
                    src_ref=stats.at[at],
                    dst_ref=landed.at[slot],
                    send_sem=stat_send.at[slot],
                    recv_sem=stat_recv.at[slot],
                    device_id=peer(mask),
                    device_id_type=MESH,
                )
            )
            copies[-1].start()
            slot += 1
        for copy in copies:
            copy.wait_recv()
        held = [stats.at[at]] + [landed.at[slot - len(stage) + i] for i in range(len(stage))]
        merged = stats.at[at + 1]
        merged[pl.ds(0, n), :] = log_add([ref[pl.ds(0, n), :] for ref in held])
        merged[pl.ds(n, 8), :] = plain_add([ref[pl.ds(n, 8), :] for ref in held])
        for copy in copies:
            copy.wait_send()

    final = stats.at[len(stages)]
    loss = (jnp.sum(final[pl.ds(0, n), :]) - jnp.sum(final[pl.ds(n, 8), :])) * (1.0 / (n * R))
    loss_ref[...] = jnp.full(loss_ref.shape, loss, jnp.float32)

    chunk = weights.shape[0]

    def backward(i, carry):
        start = pl.multiple_of(i * chunk, chunk)
        for b in range(n):
            part = jnp.exp(logits[b, pl.ds(start, chunk), :] - final[pl.ds(b, 1), :])
            hit = is_target(b, start, chunk)
            weights[:, pl.ds(b * R, R)] = jnp.where(hit, part - 1.0, part).astype(jnp.bfloat16)
        grad_ref[pl.ds(start, chunk), :] = jnp.dot(
            weights[...], rows_all[...], preferred_element_type=jnp.float32
        )
        return carry

    lax.fori_loop(0, K // chunk, backward, 0)

    def drain(j, carry):
        for p in range(2):
            ring_copy(rows(dp, core, p), dp, j, p, right).wait_send()
            pair_copy(dp, j, p, core).wait_send()
        return carry

    lax.fori_loop(1, n, drain, 0)


def shards(query_emb, positive_list, centroids, first_moment, second_moment):
    n, count_mp = lax.axis_size("dp"), lax.axis_size("mp")
    R, D = query_emb.shape
    K = centroids.shape[0]
    stages = merge_stages(n, count_mp)
    slots = sum(len(stage) for stage in stages)
    chunk = min(K, 256)
    vmem = pl.BlockSpec(memory_space=pltpu.VMEM)
    hbm = pl.BlockSpec(memory_space=pltpu.HBM)
    gradient, loss = pl.pallas_call(
        functools.partial(kernel, n, count_mp, stages),
        out_shape=(
            jax.ShapeDtypeStruct((K, D), jnp.float32),
            jax.ShapeDtypeStruct((1, 1), jnp.float32),
        ),
        in_specs=[hbm, vmem, hbm],
        out_specs=(vmem, vmem),
        scratch_shapes=[
            pltpu.VMEM((n * R, D), jnp.bfloat16),
            pltpu.VMEM((n, K, R), jnp.float32),
            pltpu.VMEM((K, D), jnp.float32),
            pltpu.VMEM((K, D), jnp.bfloat16),
            pltpu.VMEM((chunk, n * R), jnp.bfloat16),
            pltpu.VMEM((len(stages) + 1, n + 8, R), jnp.float32),
            pltpu.VMEM((slots, n + 8, R), jnp.float32),
            pltpu.SemaphoreType.DMA,
            pltpu.SemaphoreType.DMA,
            pltpu.SemaphoreType.DMA((n, 2)),
            pltpu.SemaphoreType.DMA((n, 2)),
            pltpu.SemaphoreType.DMA((n, 2)),
            pltpu.SemaphoreType.DMA((n, 2)),
            pltpu.SemaphoreType.DMA((slots,)),
            pltpu.SemaphoreType.DMA((slots,)),
        ],
        compiler_params=pltpu.CompilerParams(
            collective_id=0, has_side_effects=True, vmem_limit_bytes=36 * 2**20
        ),
        cost_estimate=pl.CostEstimate(
            flops=4 * n * R * K * D, bytes_accessed=8 * K * D, transcendentals=2 * n * R * K
        ),
        name="gather_softmax_gradient",
    )(pltpu.with_memory_space_constraint(query_emb, pltpu.HBM), positive_list.reshape(n, R), pltpu.with_memory_space_constraint(centroids, pltpu.HBM))
    new_centroids, new_first, new_second = adam_update(
        centroids, first_moment, second_moment, gradient
    )
    return (new_centroids, new_first, new_second, loss[0, 0])


def solution(mesh):
    in_specs = (
        P("dp", None),
        P(),
        P(("dp", "mp"), None),
        P(("dp", "mp"), None),
        P(("dp", "mp"), None),
    )
    out_specs = (P(("dp", "mp"), None), P(("dp", "mp"), None), P(("dp", "mp"), None), P())
    return jax.shard_map(shards, mesh=mesh, in_specs=in_specs, out_specs=out_specs, check_vma=False)
```

```python
import functools

import jax
import jax.numpy as jnp
from jax import lax
from jax.experimental import pallas as pl
from jax.experimental.pallas import tpu as pltpu
from jax.sharding import PartitionSpec as P

beta_first = 0.9
beta_second = 0.95
learn_rate = 0.01
epsilon = 1e-08

MESH = pl.DeviceIdType.MESH


def adam_update(centroids, first_moment, second_moment, gradient):
    new_first = beta_first * first_moment + (1.0 - beta_first) * gradient
    new_second = beta_second * second_moment + (1.0 - beta_second) * gradient * gradient
    new_centroids = centroids - learn_rate * new_first / (jnp.sqrt(new_second) + epsilon)
    return (new_centroids, new_first, new_second)


def merge_stages(count_dp, count_mp):
    bits = [("mp", 1 << b) for b in range(count_mp.bit_length() - 1)]
    bits += [("dp", 1 << b) for b in range(count_dp.bit_length() - 1)]
    stages = [bits[:1]]
    for at in range(1, len(bits), 2):
        stages.append(bits[at : at + 2])
    return [
        [stage[:1]] if len(stage) == 1 else [stage[:1], stage[1:], stage] for stage in stages
    ]


def flip(index, bit):
    return index + (1 - 2 * lax.rem(lax.div(index, bit), 2)) * bit


def log_add(values):
    top = functools.reduce(jnp.maximum, values)
    terms = [jnp.exp(value - top) for value in values]
    while len(terms) > 1:
        terms = [terms[i] + terms[i + 1] for i in range(0, len(terms), 2)]
    return top + jnp.log(terms[0])


def plain_add(terms):
    while len(terms) > 1:
        terms = [terms[i] + terms[i + 1] for i in range(0, len(terms), 2)]
    return terms[0]


def kernel(
    n,
    count_mp,
    stages,
    q_ref,
    pos_ref,
    cent_ref,
    grad_ref,
    loss_ref,
    rows_all,
    logits,
    cent,
    table,
    weights,
    stats,
    landed,
    cent_sem,
    own_sem,
    ring_send,
    ring_recv,
    pair_send,
    pair_recv,
    stat_send,
    stat_recv,
):
    R, D = q_ref.shape
    K = cent_ref.shape[0]
    half = R // 2
    piece = half // 2
    dp = lax.axis_index("dp")
    mp = lax.axis_index("mp")
    core = lax.rem(mp, 2)
    other = mp + 1 - 2 * core
    odd = lax.rem(dp, 2)
    place = (1 - odd) * lax.div(dp, 2) + odd * (n - 1 - lax.div(dp, 2))

    def at_place(p):
        back = lax.div(p, n // 2)
        return (1 - back) * 2 * p + back * (2 * (n - 1 - p) + 1)

    right = at_place(lax.rem(place + 1, n))
    left = at_place(lax.rem(place + n - 1, n))

    cent_copy = pltpu.make_async_copy(cent_ref, cent, cent_sem)
    own_rows = rows_all.at[pl.ds(pl.multiple_of(dp * R, R), R)]
    own_copy = pltpu.make_async_copy(q_ref, own_rows, own_sem)
    own_copy.start()
    cent_copy.start()

    def peer(mask):
        ids = {"dp": dp, "mp": mp}
        for axis, bit in mask:
            ids[axis] = flip(ids[axis], bit)
        return ids

    greeted = [{"dp": left, "mp": mp}, {"dp": right, "mp": mp}]
    greeted += [peer(mask) for stage in stages for mask in stage]
    barrier = pltpu.get_barrier_semaphore()
    for device in greeted:
        pl.semaphore_signal(barrier, inc=1, device_id=device, device_id_type=MESH)
    pl.semaphore_wait(barrier, len(greeted))

    def rows(origin, which, p):
        start = pl.multiple_of(origin * R + which * half + p * piece, piece)
        return rows_all.at[pl.ds(start, piece)]

    def ring_copy(src, origin, j, p, target):
        return pltpu.make_async_remote_copy(
            src_ref=src,
            dst_ref=rows(origin, core, p),
            send_sem=ring_send.at[j, p],
            recv_sem=ring_recv.at[j, p],
            device_id={"dp": target, "mp": mp},
            device_id_type=MESH,
        )

    def pair_copy(origin, j, p, which):
        block = rows(origin, which, p)
        return pltpu.make_async_remote_copy(
            src_ref=block,
            dst_ref=block,
            send_sem=pair_send.at[j, p],
            recv_sem=pair_recv.at[j, p],
            device_id={"dp": dp, "mp": other},
            device_id_type=MESH,
        )

    own_copy.wait()
    for p in range(2):
        own = rows(dp, core, p)
        ring_copy(own, dp, 1, p, right).start()
        ring_copy(own, dp, 2, p, left).start()

    base = (dp * count_mp + mp) * K
    first = stats.at[0]
    first[pl.ds(n, 8), :] = jnp.zeros((8, R), jnp.float32)

    def is_target(origin, start, size):
        local = pos_ref[pl.ds(origin, 1), :] - (base + start)
        return lax.broadcasted_iota(jnp.int32, (size, R), 0) == local

    step_rows = min(K, 256)

    def forward(origin):
        block = rows_all[pl.ds(pl.multiple_of(origin * R, R), R), :]
        found = lax.dot_general(
            table[...], block, (((1,), (1,)), ((), ())), preferred_element_type=jnp.float32
        )
        logits[origin] = found
        peak = jnp.max(found, axis=0, keepdims=True)
        mass = jnp.zeros((1, R), jnp.float32)
        target = jnp.zeros((1, R), jnp.float32)
        for start in range(0, K, step_rows):
            part = logits[origin, pl.ds(start, step_rows), :]
            mass += jnp.sum(jnp.exp(part - peak), axis=0, keepdims=True)
            target += jnp.sum(
                jnp.where(is_target(origin, start, step_rows), part, 0.0), axis=0, keepdims=True
            )
        first[pl.ds(origin, 1), :] = peak + jnp.log(mass)
        first[pl.ds(n, 1), :] += target

    cent_copy.wait()
    for start in range(0, K, step_rows):
        table[pl.ds(start, step_rows), :] = cent[pl.ds(start, step_rows), :].astype(jnp.bfloat16)

    forward(dp)
    far = n // 2

    def ring_step(d, carry):
        from_left = at_place(lax.rem(place - d + n, n))
        from_right = at_place(lax.rem(place + d, n))
        jl, jr = 2 * d - 1, 2 * d
        for p in range(2):
            block = rows(from_left, core, p)
            ring_copy(block, from_left, jl, p, right).wait_recv()
            onward = ring_copy(block, from_left, 2 * d + 1, p, right)
            if p == 0:
                onward.start()
            else:
                pl.when(d + 1 < far)(onward.start)
            pair_copy(from_left, jl, p, core).start()

            block = rows(from_right, core, p)
            ring_copy(block, from_right, jr, p, left).wait_recv()
            onward = ring_copy(
                block, from_right, 2 * d + 2 - p * lax.div(d + 1, far), p, left
            )
            if p == 1:
                onward.start()
            else:
                pl.when(d + 1 < far)(onward.start)
            pair_copy(from_right, jr, p, core).start()
        for p in range(2):
            pair_copy(from_left, jl, p, 1 - core).wait_recv()
            pair_copy(from_right, jr, p, 1 - core).wait_recv()
        forward(from_left)
        forward(from_right)
        return carry

    lax.fori_loop(1, far, ring_step, 0)

    last = at_place(lax.rem(place + far, n))
    for p in range(2):
        ring_copy(rows(last, core, p), last, n - 1, p, right).wait_recv()
        pair_copy(last, n - 1, p, core).start()
    for p in range(2):
        pair_copy(last, n - 1, p, 1 - core).wait_recv()
    forward(last)

    slot = 0
    for at, stage in enumerate(stages):
        copies = []
        for mask in stage:
            copies.append(
                pltpu.make_async_remote_copy(
                    src_ref=stats.at[at],
                    dst_ref=landed.at[slot],
                    send_sem=stat_send.at[slot],
                    recv_sem=stat_recv.at[slot],
                    device_id=peer(mask),
                    device_id_type=MESH,
                )
            )
            copies[-1].start()
            slot += 1
        for copy in copies:
            copy.wait_recv()
        held = [stats.at[at]] + [landed.at[slot - len(stage) + i] for i in range(len(stage))]
        merged = stats.at[at + 1]
        merged[pl.ds(0, n), :] = log_add([ref[pl.ds(0, n), :] for ref in held])
        merged[pl.ds(n, 8), :] = plain_add([ref[pl.ds(n, 8), :] for ref in held])
        for copy in copies:
            copy.wait_send()

    final = stats.at[len(stages)]
    loss = (jnp.sum(final[pl.ds(0, n), :]) - jnp.sum(final[pl.ds(n, 8), :])) * (1.0 / (n * R))
    loss_ref[...] = jnp.full(loss_ref.shape, loss, jnp.float32)

    chunk = weights.shape[0]

    def backward(i, carry):
        start = pl.multiple_of(i * chunk, chunk)
        for b in range(n):
            part = jnp.exp(logits[b, pl.ds(start, chunk), :] - final[pl.ds(b, 1), :])
            hit = is_target(b, start, chunk)
            weights[:, pl.ds(b * R, R)] = jnp.where(hit, part - 1.0, part).astype(jnp.bfloat16)
        grad_ref[pl.ds(start, chunk), :] = jnp.dot(
            weights[...], rows_all[...], preferred_element_type=jnp.float32
        )
        return carry

    lax.fori_loop(0, K // chunk, backward, 0)

    def drain(j, carry):
        for p in range(2):
            ring_copy(rows(dp, core, p), dp, j, p, right).wait_send()
            pair_copy(dp, j, p, core).wait_send()
        return carry

    lax.fori_loop(1, n, drain, 0)


def shards(query_emb, positive_list, centroids, first_moment, second_moment):
    n, count_mp = lax.axis_size("dp"), lax.axis_size("mp")
    R, D = query_emb.shape
    K = centroids.shape[0]
    stages = merge_stages(n, count_mp)
    slots = sum(len(stage) for stage in stages)
    chunk = min(K, 512)
    vmem = pl.BlockSpec(memory_space=pltpu.VMEM)
    hbm = pl.BlockSpec(memory_space=pltpu.HBM)
    gradient, loss = pl.pallas_call(
        functools.partial(kernel, n, count_mp, stages),
        out_shape=(
            jax.ShapeDtypeStruct((K, D), jnp.float32),
            jax.ShapeDtypeStruct((1, 1), jnp.float32),
        ),
        in_specs=[hbm, vmem, hbm],
        out_specs=(vmem, vmem),
        scratch_shapes=[
            pltpu.VMEM((n * R, D), jnp.bfloat16),
            pltpu.VMEM((n, K, R), jnp.float32),
            pltpu.VMEM((K, D), jnp.float32),
            pltpu.VMEM((K, D), jnp.bfloat16),
            pltpu.VMEM((chunk, n * R), jnp.bfloat16),
            pltpu.VMEM((len(stages) + 1, n + 8, R), jnp.float32),
            pltpu.VMEM((slots, n + 8, R), jnp.float32),
            pltpu.SemaphoreType.DMA,
            pltpu.SemaphoreType.DMA,
            pltpu.SemaphoreType.DMA((n, 2)),
            pltpu.SemaphoreType.DMA((n, 2)),
            pltpu.SemaphoreType.DMA((n, 2)),
            pltpu.SemaphoreType.DMA((n, 2)),
            pltpu.SemaphoreType.DMA((slots,)),
            pltpu.SemaphoreType.DMA((slots,)),
        ],
        compiler_params=pltpu.CompilerParams(
            collective_id=0, has_side_effects=True, vmem_limit_bytes=36 * 2**20
        ),
        cost_estimate=pl.CostEstimate(
            flops=4 * n * R * K * D, bytes_accessed=8 * K * D, transcendentals=2 * n * R * K
        ),
        name="gather_softmax_gradient",
    )(pltpu.with_memory_space_constraint(query_emb, pltpu.HBM), positive_list.reshape(n, R), pltpu.with_memory_space_constraint(centroids, pltpu.HBM))
    new_centroids, new_first, new_second = adam_update(
        centroids, first_moment, second_moment, gradient
    )
    return (new_centroids, new_first, new_second, loss[0, 0])


def solution(mesh):
    in_specs = (
        P("dp", None),
        P(),
        P(("dp", "mp"), None),
        P(("dp", "mp"), None),
        P(("dp", "mp"), None),
    )
    out_specs = (P(("dp", "mp"), None), P(("dp", "mp"), None), P(("dp", "mp"), None), P())
    return jax.shard_map(shards, mesh=mesh, in_specs=in_specs, out_specs=out_specs, check_vma=False)
```
